128 devices in a mesh: blk: 8 (over x, y_lo), uly: 2 (over core), dp: 8 (over z, y_hi).
Axes of the slice: x: 4, y: 4 (y_hi: 2, y_lo: 2; y = y_hi * 2 + y_lo), z: 4, core: 2. Of those that a mesh axis runs over, the one named last changes fastest.
Arguments:
- short_tokens: bfloat16 [64, 1024, 4096], P(('blk', 'dp'), 'uly'), may hold values from -150 to 150, as said below
- short_segments: int32 [64, 1024], P(('blk', 'dp')), may hold values from 0 to 3, never falling along the last dimension, each value on 1 to 512 neighbouring positions
- long_tokens: bfloat16 [8, 3072, 4096], P('dp', 'blk'), may hold values from -150 to 150, as said below
- long_lengths: int32 [8], P('dp'), may hold values from 768 to 3072
- w_query: bfloat16 [4096, 2048], P(('blk', 'dp'), 'uly'), may hold values from -0.09375 to 0.09375
- w_key: bfloat16 [4096, 512], P(('blk', 'dp'), 'uly'), may hold values from -0.09375 to 0.09375
- w_value: bfloat16 [4096, 512], P(('blk', 'dp'), 'uly'), may hold values from -0.09375 to 0.09375
Outputs:
- short_out: bfloat16 [64, 1024, 2048], P(('blk', 'dp'), 'uly')
- long_out: bfloat16 [8, 3072, 2048], P('dp', 'blk', 'uly')
The draws below stay inside these ranges and needn't reach their ends.
Inputs may be any that keep to these rules, and one draw needn't show every extreme that they name: `short_tokens`: activations of the short bucket. `long_tokens`: activations of the long bucket; rows at or after a sequence's length are padding. `short_segments`: document numbers never fall along a sequence. `long_lengths`: a long sequence occupies positions 0 to its length - 1 of its 3072 slots.
All inputs are finite; a program needn't handle non-finite values.
Results may differ from the reference program's by a relative error of at most 0.012.
The reference program's roundings to bfloat16 on the way count: a program that leaves them out, or rounds other values in their place, can miss the bound.
Values may be sent and summed in bfloat16 or wider, within the bound.
No kernel may reach another device: no remote copies, remote signals or barrier semaphores. Data moves between devices by JAX's collectives and lax.ppermute only.
A program may use at most 128 MiB of HBM per device.

```python
import math
import jax
import jax.numpy as jnp
import numpy as np
from jax import lax

D = 4096
HQ = 16
HK = 4
HD = 128
LS = 1024
NS = 64
NL = 8
LL = 3072


def token_rows(key, shape):
    base = jnp.clip(jax.random.normal(key, shape, jnp.float32), -6.0, 6.0)
    return base.astype(jnp.bfloat16)


def draw_short_tokens(key, part):
    return token_rows(jax.random.fold_in(key, 101), (NS, LS, D))


def draw_long_tokens(key, part):
    return token_rows(jax.random.fold_in(key, 202), (NL, LL, D))


def plant(values, stream_key, low, largest):
    place = [jax.random.randint(jax.random.fold_in(stream_key, axis), (), 0, length) for axis, length in enumerate(values.shape)]
    longest = values.shape.index(max(values.shape))
    neighbour = place[:longest] + [(place[longest] + 1) % values.shape[longest]] + place[longest + 1:]
    return values.at[tuple(place)].set(low).at[tuple(neighbour)].set(largest)


def levels(rng, dims, shards, least, top_value):
    def one(dim, blocks):
        heights = jax.random.uniform(jax.random.fold_in(jax.random.fold_in(rng, 6), dim), (blocks,), jnp.float32, least / len(shards), top_value / len(shards))
        return jnp.repeat(jnp.exp(heights), dims[dim] // blocks).reshape((-1,) + (1,) * (len(dims) - dim - 1))

    loudness = one(*shards[0])
    for cut in shards[1:]:
        loudness = loudness * one(*cut)
    return loudness


def length_profile(number_of, total, most, lean):
    weights = [(1 << 20) // math.isqrt(grade ** lean) + 1 for grade in range(2, number_of + 1)]
    spare, counts = total - most - (number_of - 1), [1] * (number_of - 1)
    while spare > 0:
        movable = [i for i in range(number_of - 1) if counts[i] < most]
        whole, remaining = sum([weights[i] for i in movable]), spare
        for i in movable:
            extra = min(most - counts[i], max(1, remaining * weights[i] // whole), spare)
            counts[i] = counts[i] + extra
            spare = spare - extra
    return np.array([most] + counts)


def uneven(own_key, number_of, total, most, lean):
    if number_of == 2:
        one = jax.random.randint(own_key, (), max(1, total - most), min(most, total - 1) + 1)
        return jnp.stack([one, total - one])
    lengths = jnp.asarray(length_profile(number_of, total, most, lean), jnp.int32)
    twos = (number_of - 1) // 2
    donor, receiver = lengths[1:1 + 2 * twos:2], lengths[2:2 + 2 * twos:2]
    room = jnp.minimum(donor - 1, most - receiver)
    shifted = jax.random.randint(jax.random.fold_in(own_key, 1), (twos,), 0, 1 << 20) % (room + 1)
    lengths = lengths.at[1:1 + 2 * twos:2].set(donor - shifted).at[2:2 + 2 * twos:2].set(receiver + shifted)
    return lengths[jax.random.permutation(jax.random.fold_in(own_key, 2), number_of)]


def gaussian(own_key, extent, width, bound, split=(), kind=jnp.bfloat16):
    factor_of = levels(own_key, extent, split, -0.22, 0.18) if split else 1.0
    drawn = jax.random.normal(own_key, extent, jnp.float32) * width * factor_of
    return jnp.minimum(jnp.maximum(drawn, -bound), bound).astype(kind)


def setup_inputs(seed: int = 0) -> dict:
    keys = jax.random.split(jax.random.key(seed), 8)
    short_tokens = draw_short_tokens(jax.random.fold_in(keys[7], 71), 0)
    short_segments = jax.vmap(lambda own: jnp.searchsorted(jnp.cumsum(uneven(own, 4, LS, LS // 2, 1)), jnp.arange(LS), side="right"))(jax.random.split(keys[1], NS)).reshape((NS, LS)).astype(jnp.int32)
    long_tokens = draw_long_tokens(jax.random.fold_in(keys[7], 71), 0)
    long_lengths = plant(jax.random.randint(keys[3], (NL,), LL // 4, LL + 1), jax.random.fold_in(keys[3], 1), LL // 4, LL).astype(jnp.int32)
    w_query = gaussian(keys[4], (D, HQ * HD), D ** -0.5, 0.09375, ((0, 64), (1, 2)))
    w_key = gaussian(keys[5], (D, HK * HD), D ** -0.5, 0.09375, ((0, 64), (1, 2)))
    w_value = gaussian(keys[6], (D, HK * HD), D ** -0.5, 0.09375, ((0, 64), (1, 2)))
    return {"short_tokens": short_tokens, "short_segments": short_segments, "long_tokens": long_tokens, "long_lengths": long_lengths, "w_query": w_query, "w_key": w_key, "w_value": w_value}


masked_score = -1e+30

def rounded_wide(array):
    return lax.optimization_barrier(array.astype(jnp.bfloat16)).astype(jnp.float32)

def project(rows, weight):
    return jnp.dot(rows, weight, preferred_element_type=jnp.float32)

def attention(queries, key_rows, value_rows, visible_rows):
    seq_len = key_rows.shape[0]
    block_rows = min(512, seq_len)
    group_size = HQ // HK
    key_heads = key_rows.reshape(seq_len, HK, HD)
    value_heads = value_rows.reshape(seq_len, HK, HD)
    outputs = []
    for block_index in range(seq_len // block_rows):
        first_row = block_index * block_rows
        query_heads = queries[first_row:first_row + block_rows].reshape(block_rows, HK, group_size, HD)
        visible = visible_rows(first_row, block_rows)
        scores = jnp.einsum('bhgd,khd->hgbk', query_heads, key_heads) * (1.0 / math.sqrt(HD))
        scores = jnp.where(visible, scores, masked_score)
        row_max = lax.optimization_barrier(jnp.max(scores, axis=-1, keepdims=True))
        exponentials = jnp.where(visible, jnp.exp(scores - row_max), 0.0)
        totals = lax.optimization_barrier(jnp.sum(exponentials, axis=-1))
        mixed = jnp.einsum('hgbk,khd->hgbd', rounded_wide(exponentials), value_heads)
        mixed = mixed / totals[..., None]
        outputs.append(jnp.transpose(mixed, (2, 0, 1, 3)).reshape(block_rows, HQ * HD))
    return jnp.concatenate(outputs, axis=0)

def reference(short_tokens, short_segments, long_tokens, long_lengths, w_query, w_key, w_value):

    def one_short(inputs):
        rows, segments = inputs
        queries = rounded_wide(project(rows, w_query))
        key_rows = rounded_wide(project(rows, w_key))
        value_rows = rounded_wide(project(rows, w_value))
        positions = jnp.arange(rows.shape[0], dtype=jnp.int32)

        def visible_rows(first_row, block_rows):
            query_pos = positions[first_row:first_row + block_rows]
            query_seg = segments[first_row:first_row + block_rows]
            return (positions[None, :] <= query_pos[:, None]) & (segments[None, :] == query_seg[:, None])
        mixed = attention(queries, key_rows, value_rows, visible_rows)
        return mixed.astype(jnp.bfloat16)

    def one_long(inputs):
        rows, length = inputs
        queries = rounded_wide(project(rows, w_query))
        key_rows = rounded_wide(project(rows, w_key))
        value_rows = rounded_wide(project(rows, w_value))
        positions = jnp.arange(rows.shape[0], dtype=jnp.int32)

        def visible_rows(first_row, block_rows):
            query_pos = positions[first_row:first_row + block_rows]
            return (positions[None, :] <= query_pos[:, None]) & (positions[None, :] < length)
        mixed = attention(queries, key_rows, value_rows, visible_rows)
        mixed = jnp.where(positions[:, None] < length, mixed, 0.0)
        return mixed.astype(jnp.bfloat16)
    short_out = lax.map(one_short, (short_tokens, short_segments))
    long_out = lax.map(one_long, (long_tokens, long_lengths))
    return (short_out, long_out)
```

```python
import math

import jax
import jax.numpy as jnp
from jax import lax
from jax.sharding import PartitionSpec as P

HD = 128


masked_score = -1e30


def torus_order():
    return [
        (x * 2 + y % 2) * 8 + z * 2 + y // 2 for x in range(4) for z in range(4) for y in range(4)
    ]


def gathered_weights(arrays):
    both = jnp.concatenate(arrays, axis=1)
    whole = lax.all_gather(
        both, ("blk", "dp"), axis=0, tiled=True, axis_index_groups=[torus_order()]
    )
    rows = both.shape[0]
    whole = whole.reshape(4, 4, 2, 2, rows, both.shape[1])
    whole = jnp.transpose(whole, (0, 3, 1, 2, 4, 5)).reshape(64 * rows, both.shape[1])
    at, outs = 0, []
    for a in arrays:
        outs.append(lax.slice_in_dim(whole, at, at + a.shape[1], axis=1))
        at += a.shape[1]
    return tuple(outs)


def side_by_side(arrays, axis, dim, along):
    both = jnp.concatenate(arrays, axis=along)
    whole, at, outs = (lax.all_gather(both, axis, axis=dim, tiled=True), 0, [])
    for a in arrays:
        outs.append(lax.slice_in_dim(whole, at, at + a.shape[along], axis=along))
        at += a.shape[along]
    return tuple(outs)


def head_scores(query_rows, key_rows, kv_heads):
    query_heads = query_rows.reshape(query_rows.shape[0], kv_heads, -1, HD)
    key_heads = key_rows.reshape(key_rows.shape[0], kv_heads, HD)
    scores = jnp.einsum(
        "bhgd,khd->hgbk", query_heads, key_heads, preferred_element_type=jnp.float32
    )
    return scores * (1.0 / math.sqrt(HD))


def weighted_values(probabilities, value_rows, kv_heads):
    value_heads = value_rows.reshape(value_rows.shape[0], kv_heads, HD)
    return jnp.einsum(
        "hgbk,khd->hgbd", probabilities, value_heads, preferred_element_type=jnp.float32
    )


def short_attention(queries, key_rows, value_rows, segments):
    kv_heads = key_rows.shape[1] // HD
    seq_len = key_rows.shape[0]
    block_rows = min(512, seq_len)
    positions = jnp.arange(seq_len, dtype=jnp.int32)
    outputs = []
    for block_index in range(seq_len // block_rows):
        first_row = block_index * block_rows
        query_pos = positions[first_row : first_row + block_rows]
        query_seg = segments[first_row : first_row + block_rows]
        visible = (positions[None, :] <= query_pos[:, None]) & (
            segments[None, :] == query_seg[:, None]
        )
        scores = head_scores(queries[first_row : first_row + block_rows], key_rows, kv_heads)
        scores = jnp.where(visible, scores, masked_score)
        row_max = jnp.max(scores, axis=-1, keepdims=True)
        exponentials = jnp.where(visible, jnp.exp(scores - row_max), 0.0)
        totals = jnp.sum(exponentials, axis=-1)
        mixed = (
            weighted_values(exponentials.astype(jnp.bfloat16), value_rows, kv_heads)
            / totals[..., None]
        )
        outputs.append(jnp.transpose(mixed, (2, 0, 1, 3)).reshape(block_rows, -1))
    return jnp.concatenate(outputs, axis=0).astype(jnp.bfloat16)


def local(short_tokens, short_segments, long_tokens, long_lengths, w_query, w_key, w_value):
    short_rows = short_tokens[0]
    long_rows = long_tokens[0]
    long_count = long_rows.shape[0]
    query_cols = w_query.shape[1]
    kv_cols = w_key.shape[1]
    partner_rows = lax.ppermute(short_rows, "uly", [(0, 1), (1, 0)])
    first = lax.axis_index("uly") == 0
    whole_rows = jnp.concatenate(
        [jnp.where(first, short_rows, partner_rows), jnp.where(first, partner_rows, short_rows)]
    )
    pieces = gathered_weights((w_query, w_key, w_value))
    short_new = tuple(
        (jnp.dot(whole_rows, pieces[i], preferred_element_type=jnp.float32) for i in range(3))
    )
    long_new = tuple(
        (jnp.dot(long_rows, pieces[i], preferred_element_type=jnp.float32) for i in range(3))
    )
    projected = short_new + long_new
    query_short, key_short, value_short = tuple(
        (item.astype(jnp.bfloat16) for item in projected[:3])
    )
    query_long, key_long, value_long = tuple((item.astype(jnp.bfloat16) for item in projected[3:]))
    attended = short_attention(query_short, key_short, value_short, short_segments[0])
    short_back = lax.all_to_all(attended, "uly", split_axis=0, concat_axis=1, tiled=True)
    long_len = long_lengths[0]
    query_pos = lax.axis_index("blk") * long_count + jnp.arange(long_count, dtype=jnp.int32)
    kv_heads = kv_cols // HD
    group_size = query_cols // kv_cols
    cycle_init = (
        jnp.full((kv_heads, group_size, long_count), masked_score, jnp.float32),
        jnp.zeros((kv_heads, group_size, long_count), jnp.float32),
        jnp.zeros((kv_heads, group_size, long_count, HD), jnp.float32),
    )
    carry = cycle_init
    key_piece, value_piece = side_by_side((key_long, value_long), "blk", 0, 1)
    piece_rows = key_piece.shape[0]
    block_rows = math.gcd(piece_rows, 512)
    blocks_count = piece_rows // block_rows
    key_blocks = key_piece.reshape(blocks_count, block_rows, -1)
    value_blocks = value_piece.reshape(blocks_count, block_rows, -1)
    block_starts = block_rows * jnp.arange(blocks_count, dtype=jnp.int32)

    def update(states, block_key, block_value, block_start):
        running_max, running_sum, accumulated = states
        key_pos = block_start + jnp.arange(block_rows, dtype=jnp.int32)
        visible = (key_pos[None, :] <= query_pos[:, None]) & (key_pos[None, :] < long_len)
        scores = jnp.where(visible, head_scores(query_long, block_key, kv_heads), masked_score)
        new_max = jnp.maximum(running_max, jnp.max(scores, axis=-1))
        rescale = jnp.exp(running_max - new_max)
        exponentials = jnp.where(visible, jnp.exp(scores - new_max[..., None]), 0.0)
        running_sum = running_sum * rescale + jnp.sum(exponentials, axis=-1)
        accumulated = accumulated * rescale[..., None] + weighted_values(
            exponentials.astype(jnp.bfloat16), block_value, kv_heads
        )
        return (new_max, running_sum, accumulated)

    def advance(states, inputs):
        block_key, block_value, block_start = inputs
        needed = (block_start <= query_pos[-1]) & (block_start < long_len)
        states = lax.cond(
            needed,
            lambda current: update(current, block_key, block_value, block_start),
            lambda current: current,
            states,
        )
        return (states, None)

    carry, unused = lax.scan(advance, carry, (key_blocks, value_blocks, block_starts))
    running_max, running_sum, accumulated = carry
    mixed = accumulated / running_sum[..., None]
    mixed = jnp.transpose(mixed, (2, 0, 1, 3)).reshape(long_count, query_cols)
    mixed = jnp.where(query_pos[:, None] < long_len, mixed, 0.0)
    return (short_back[None], mixed.astype(jnp.bfloat16)[None])


def solution(mesh):
    return jax.shard_map(
        local,
        mesh=mesh,
        in_specs=(
            P(("blk", "dp"), "uly", None),
            P(("blk", "dp"), None),
            P("dp", "blk", None),
            P("dp"),
            P(("blk", "dp"), "uly"),
            P(("blk", "dp"), "uly"),
            P(("blk", "dp"), "uly"),
        ),
        out_specs=(P(("blk", "dp"), "uly", None), P("dp", "blk", "uly")),
        check_vma=False,
    )
```

```python
import math

import jax
import jax.numpy as jnp
from jax import lax
from jax.experimental import pallas as pl
from jax.experimental.pallas import tpu as pltpu
from jax.sharding import PartitionSpec as P

HD = 128
HIDDEN = -1e30
EXP_SCALE = math.log2(math.e) / math.sqrt(HD)
VMEM = pltpu.VMEM


def torus_order():
    return [
        (x * 2 + y % 2) * 8 + z * 2 + y // 2 for x in range(4) for z in range(4) for y in range(4)
    ]


def blk_order():
    return [x * 2 + y_lo for y_lo in range(2) for x in range(4)]


def project_tile(tokens, weights):
    total = None
    for part in range(8):
        x, y_lo = part // 2, part % 2
        rows = weights[x, :, :, y_lo].reshape(512, weights.shape[-1])
        term = jnp.dot(
            tokens[:, 512 * part : 512 * (part + 1)], rows, preferred_element_type=jnp.float32
        )
        total = term if total is None else total + term
    return total.astype(jnp.bfloat16)


def long_kv_kernel(tokens, weights, out):
    out[...] = project_tile(tokens, weights)


def project_kernel(core, own, partner, long, weights, out_short, out_long):
    first = pl.multiple_of(core[0] * 512, 512)
    out_short[pl.ds(first, 512), :] = project_tile(own, weights)
    out_short[pl.ds(512 - first, 512), :] = project_tile(partner, weights)

    @pl.when(pl.program_id(0) >= 2)
    def _():
        out_long[...] = project_tile(long, weights)


WEIGHT_BLOCK = (4, 4, 2, 2, 64, 256)


def project_long_kv(long_rows, weights):
    return pl.pallas_call(
        long_kv_kernel,
        grid=(2,),
        in_specs=[
            pl.BlockSpec(memory_space=VMEM),
            pl.BlockSpec(WEIGHT_BLOCK, lambda n: (0, 0, 0, 0, 0, n)),
        ],
        out_specs=pl.BlockSpec((384, 256), lambda n: (0, n)),
        out_shape=jax.ShapeDtypeStruct((384, 512), jnp.bfloat16),
        compiler_params=pltpu.CompilerParams(vmem_limit_bytes=24 << 20),
        cost_estimate=pl.CostEstimate(
            flops=2 * 384 * 4096 * 512, bytes_accessed=8 << 20, transcendentals=0
        ),
    )(long_rows, weights)


def project_rest(core, own, partner, long_rows, weights):
    return pl.pallas_call(
        project_kernel,
        grid_spec=pltpu.PrefetchScalarGridSpec(
            num_scalar_prefetch=1,
            grid=(6,),
            in_specs=[
                pl.BlockSpec(memory_space=VMEM),
                pl.BlockSpec(memory_space=VMEM),
                pl.BlockSpec(memory_space=VMEM),
                pl.BlockSpec(WEIGHT_BLOCK, lambda n, core: (0, 0, 0, 0, 0, n)),
            ],
            out_specs=[
                pl.BlockSpec((1024, 256), lambda n, core: (0, n)),
                pl.BlockSpec((384, 256), lambda n, core: (0, jnp.maximum(n - 2, 0))),
            ],
        ),
        out_shape=[
            jax.ShapeDtypeStruct((1024, 1536), jnp.bfloat16),
            jax.ShapeDtypeStruct((384, 1024), jnp.bfloat16),
        ],
        compiler_params=pltpu.CompilerParams(vmem_limit_bytes=40 << 20),
        cost_estimate=pl.CostEstimate(
            flops=2 * 1408 * 4096 * 1536, bytes_accessed=24 << 20, transcendentals=0
        ),
    )(core, own, partner, long_rows, weights)


def softmax_rows(scores):
    scaled = scores * EXP_SCALE
    top = jnp.max(scaled, axis=-1, keepdims=True)
    return jnp.exp2(scaled - top)


QUERY_ROWS = 128


def short_kernel(seg_row, seg_col, queries, keys, values, out):
    for block in range(1024 // QUERY_ROWS):
        first = block * QUERY_ROWS
        start = max(0, first - 512)
        end = first + QUERY_ROWS
        width = end - start
        same = seg_col[first:end, 0:1] == seg_row[0:1, start:end]
        query_pos = first + lax.broadcasted_iota(jnp.int32, (QUERY_ROWS, width), 0)
        key_pos = start + lax.broadcasted_iota(jnp.int32, (QUERY_ROWS, width), 1)
        bias = jnp.where(same & (key_pos <= query_pos), 0.0, HIDDEN)
        key_rows = keys[start:end, :]
        value_rows = values[start:end, :]
        for head in range(4):
            scores = lax.dot_general(
                queries[first:end, head * HD : (head + 1) * HD],
                key_rows,
                (((1,), (1,)), ((), ())),
                preferred_element_type=jnp.float32,
            )
            exponentials = softmax_rows(scores + bias)
            totals = jnp.sum(exponentials, axis=-1, keepdims=True)
            mixed = jnp.dot(
                exponentials.astype(jnp.bfloat16), value_rows, preferred_element_type=jnp.float32
            )
            out[first:end, head * HD : (head + 1) * HD] = (mixed * (1.0 / totals)).astype(
                jnp.bfloat16
            )


def short_attention(segments, projected):
    seg_col = jnp.broadcast_to(segments.reshape(1024, 1), (1024, 128))
    return pl.pallas_call(
        short_kernel,
        grid=(2,),
        in_specs=[
            pl.BlockSpec((1, 1024), lambda g: (0, 0)),
            pl.BlockSpec((1024, 128), lambda g: (0, 0)),
            pl.BlockSpec((1024, 512), lambda g: (0, 1 + g)),
            pl.BlockSpec((1024, 128), lambda g: (0, g)),
            pl.BlockSpec((1024, 128), lambda g: (0, 2 + g)),
        ],
        out_specs=pl.BlockSpec((1024, 512), lambda g: (0, g)),
        out_shape=jax.ShapeDtypeStruct((1024, 1024), jnp.bfloat16),
        compiler_params=pltpu.CompilerParams(vmem_limit_bytes=24 << 20),
        cost_estimate=pl.CostEstimate(
            flops=8 * 1024 * 640 * 512, bytes_accessed=6 << 20, transcendentals=8 * 1024 * 640
        ),
    )(segments, seg_col, projected, projected, projected)


LONG_ROWS = 384


def long_kernel(place, queries, kv, out, top, total, mixed):
    block = place[0]
    length = place[1]
    first = block * LONG_ROWS
    live = first < length
    rows_shape = (LONG_ROWS, LONG_ROWS)

    def visit(index, head, diagonal):
        slot = index // 2 + 4 * (index % 2)
        at = pl.multiple_of(slot * LONG_ROWS, LONG_ROWS)
        group = head // 4
        key_rows = kv[pl.ds(at, LONG_ROWS), group * HD : (group + 1) * HD]
        value_rows = kv[pl.ds(at, LONG_ROWS), 256 + group * HD : 256 + (group + 1) * HD]
        scores = lax.dot_general(
            queries[:, head * HD : (head + 1) * HD],
            key_rows,
            (((1,), (1,)), ((), ())),
            preferred_element_type=jnp.float32,
        )
        scores = scores * EXP_SCALE
        key_pos = index * LONG_ROWS + lax.broadcasted_iota(jnp.int32, rows_shape, 1)
        visible = key_pos < length
        if diagonal:
            query_pos = first + lax.broadcasted_iota(jnp.int32, rows_shape, 0)
            visible = visible & (key_pos <= query_pos)
        scores = jnp.where(visible, scores, HIDDEN)
        old = top[head]
        new = jnp.maximum(old, jnp.max(scores, axis=-1, keepdims=True))
        rescale = jnp.exp2(old - new)
        exponentials = jnp.exp2(scores - new)
        top[head] = new
        total[head] = total[head] * rescale + jnp.sum(exponentials, axis=-1, keepdims=True)
        mixed[head] = mixed[head] * rescale + jnp.dot(
            exponentials.astype(jnp.bfloat16), value_rows, preferred_element_type=jnp.float32
        )

    @pl.when(live)
    def _():
        top[...] = jnp.full_like(top, HIDDEN)
        total[...] = jnp.zeros_like(total)
        mixed[...] = jnp.zeros_like(mixed)

        @pl.loop(0, block)
        def _(index):
            for head in range(8):
                visit(index, head, False)

        for head in range(8):
            visit(block, head, True)
        position = first + lax.broadcasted_iota(jnp.int32, (LONG_ROWS, HD), 0)
        for head in range(8):
            done = mixed[head] * (1.0 / total[head])
            out[:, head * HD : (head + 1) * HD] = jnp.where(position < length, done, 0.0).astype(
                jnp.bfloat16
            )

    @pl.when(jnp.logical_not(live))
    def _():
        out[...] = jnp.zeros_like(out)


def long_attention(place, queries, kv):
    return pl.pallas_call(
        long_kernel,
        in_specs=[
            pl.BlockSpec(memory_space=pltpu.SMEM),
            pl.BlockSpec(memory_space=VMEM),
            pl.BlockSpec(memory_space=VMEM),
        ],
        out_specs=pl.BlockSpec(memory_space=VMEM),
        out_shape=jax.ShapeDtypeStruct((LONG_ROWS, 1024), jnp.bfloat16),
        scratch_shapes=[
            VMEM((8, LONG_ROWS, 1), jnp.float32),
            VMEM((8, LONG_ROWS, 1), jnp.float32),
            VMEM((8, LONG_ROWS, HD), jnp.float32),
        ],
        compiler_params=pltpu.CompilerParams(vmem_limit_bytes=24 << 20),
        cost_estimate=pl.CostEstimate(
            flops=8 * 384 * 3072 * 512, bytes_accessed=6 << 20, transcendentals=8 * 384 * 3072
        ),
    )(place, queries, kv)


def local(short_tokens, short_segments, long_tokens, long_lengths, w_query, w_key, w_value):
    short_rows = short_tokens[0]
    long_rows = long_tokens[0]
    core = lax.axis_index("uly")
    partner_rows = lax.ppermute(short_rows, "uly", [(0, 1), (1, 0)])
    both = jnp.concatenate((w_key, w_value, w_query), axis=1)
    weights = lax.all_gather(
        both, ("blk", "dp"), axis=0, tiled=True, axis_index_groups=[torus_order()]
    ).reshape(4, 4, 2, 2, 64, 1536)
    long_kv = project_long_kv(long_rows, weights)
    kv = lax.all_gather(long_kv, "blk", axis=0, tiled=True, axis_index_groups=[blk_order()])
    core_index = core.astype(jnp.int32).reshape(1)
    projected, long_queries = project_rest(
        core_index, short_rows, partner_rows, long_rows, weights
    )
    attended = short_attention(short_segments, projected)
    mine = lax.dynamic_slice_in_dim(attended, core * 512, 512, axis=0)
    theirs = lax.dynamic_slice_in_dim(attended, 512 - core * 512, 512, axis=0)
    other = lax.ppermute(theirs, "uly", [(0, 1), (1, 0)])
    short_out = jnp.concatenate(
        [jnp.where(core == 0, mine, other), jnp.where(core == 0, other, mine)], axis=1
    )
    place = jnp.stack([lax.axis_index("blk").astype(jnp.int32), long_lengths[0]])
    long_out = long_attention(place, long_queries, kv)
    return short_out[None], long_out[None]


def solution(mesh):
    return jax.shard_map(
        local,
        mesh=mesh,
        in_specs=(
            P(("blk", "dp"), "uly", None),
            P(("blk", "dp"), None),
            P("dp", "blk", None),
            P("dp"),
            P(("blk", "dp"), "uly"),
            P(("blk", "dp"), "uly"),
            P(("blk", "dp"), "uly"),
        ),
        out_specs=(P(("blk", "dp"), "uly", None), P("dp", "blk", "uly")),
        check_vma=False,
    )
```

```python
import functools
import itertools
import math

import jax
import jax.numpy as jnp
from jax import lax
from jax.experimental import pallas as pl
from jax.experimental.pallas import tpu as pltpu
from jax.sharding import PartitionSpec as P


HD = 128
HIDDEN = -1e30
EXP_SCALE = math.log2(math.e) / math.sqrt(HD)
VMEM = pltpu.VMEM


ALL_AXES = ("blk", "uly", "dp")
QUERY_DIMS = ((2, 1, 0), (0, 2, 1))
KV_DIMS = ((1, 0, 2), (1, 0, 2))


def device_index(x, y, z, core):
    return ((x * 2 + y % 2) * 2 + core) * 8 + z * 2 + y // 2


def shift(rows, dims, hops):
    pairs = []
    for core in range(2):
        for at in itertools.product(range(4), repeat=3):
            to = list(at)
            to[dims[core]] = (to[dims[core]] + hops) % 4
            pairs.append((device_index(*at, core), device_index(*to, core)))
    return lax.ppermute(rows, ALL_AXES, pairs)


def swap_y_lo(rows):
    pairs = []
    for core in range(2):
        for x, y, z in itertools.product(range(4), repeat=3):
            pairs.append((device_index(x, y, z, core), device_index(x, y ^ 1, z, core)))
    return lax.ppermute(rows, ALL_AXES, pairs)


SMEM_SPEC = pl.BlockSpec(memory_space=pltpu.SMEM)
VMEM_SPEC = pl.BlockSpec(memory_space=VMEM)
HBM_SPEC = pl.BlockSpec(memory_space=pltpu.HBM)


def pack_kernel(parts, *refs):
    outs = refs[-len(parts) :]
    at = 0
    for out, count in zip(outs, parts):
        row = 0
        for ref in refs[at : at + count]:
            out[row : row + ref.shape[0], :] = ref[...]
            row += ref.shape[0]
        at += count


def pack(*groups):
    parts = tuple(len(group) for group in groups)
    flat = [piece for group in groups for piece in group]
    shapes = [
        jax.ShapeDtypeStruct((sum(p.shape[0] for p in group), group[0].shape[1]), jnp.bfloat16)
        for group in groups
    ]
    size = sum(piece.size for piece in flat) * 4
    return pl.pallas_call(
        functools.partial(pack_kernel, parts),
        in_specs=[VMEM_SPEC] * len(flat),
        out_specs=[VMEM_SPEC] * len(parts),
        out_shape=shapes,
        compiler_params=pltpu.CompilerParams(vmem_limit_bytes=8 << 20),
        cost_estimate=pl.CostEstimate(flops=size, bytes_accessed=size, transcendentals=0),
    )(*flat)


def direct_ring(rows, dims):
    return rows, shift(rows, dims, -1), shift(rows, dims, 2), shift(rows, dims, 1)


def passed_ring(rows, dims):
    after = shift(rows, dims, -1)
    before = shift(rows, dims, 1)
    return rows, after, shift(after, dims, -1), before


def halved_ring(low, high, dims):
    before_low = shift(low, dims, 1)
    after_high = shift(high, dims, -1)
    before_high = shift(high, dims, 1)
    after_low = shift(low, dims, -1)
    far_low = shift(before_low, dims, 1)
    far_high = shift(after_high, dims, -1)
    pieces = (low, high, after_low, after_high, far_low, far_high, before_low, before_high)
    return tuple(piece.reshape(8, 64, piece.shape[1]) for piece in pieces)


def gather_weights(w_query, kv_weights):
    query_dims, kv_dims = tuple(zip(*QUERY_DIMS)), tuple(zip(*KV_DIMS))
    queries, kv = pack(direct_ring(w_query, query_dims[0]), direct_ring(kv_weights, kv_dims[0]))
    query_four = passed_ring(queries, query_dims[1])
    kv_four = passed_ring(kv, kv_dims[1])
    query_low, query_high, kv_low, kv_high = pack(
        query_four[:2], query_four[2:], kv_four[:2], kv_four[2:]
    )
    kv_pieces = halved_ring(kv_low, kv_high, kv_dims[2])
    query_pieces = halved_ring(query_low, query_high, query_dims[2])
    return query_pieces, kv_pieces


def block_table(coords, core):
    t = jnp.arange(64, dtype=jnp.int32)
    at = (t // 16, (t % 2) * 2 + (t // 8) % 2, (t // 2) % 4)
    steps = [(a - c) & 3 for a, c in zip(at, coords)]

    def table(dims):
        return steps[dims[2]] * 16 + steps[dims[1]] * 4 + steps[dims[0]]

    queries = jnp.where(core == 0, table(QUERY_DIMS[0]), table(QUERY_DIMS[1]))
    return jnp.concatenate([queries, table(KV_DIMS[0])])


def piece_copies(pieces, held, sems):
    copies, at = [], 0
    for i, piece in enumerate(pieces):
        count = piece.shape[0]
        copies.append(pltpu.make_async_copy(piece, held.at[at : at + count], sems.at[i]))
        at += count
    return copies


def weight_rows(table, base, part, held, columns):
    return jnp.concatenate(
        [held[table[base + 8 * part + r], :, columns] for r in range(8)], axis=0
    )


def project_tile(table, base, held, columns, tokens):
    total = None
    for part in range(8):
        rows = weight_rows(table, base, part, held, columns)
        term = jnp.dot(
            tokens[:, 512 * part : 512 * (part + 1)], rows, preferred_element_type=jnp.float32
        )
        total = term if total is None else total + term
    return total.astype(jnp.bfloat16)


def load(pieces, held, sems):
    copies = piece_copies(pieces, held, sems)
    for copy in copies:
        copy.start()
    return copies


def long_kv_kernel(table, tokens, *refs):
    pieces = refs[:8]
    out, held, sems = refs[8:]
    for copy in load(pieces, held, sems):
        copy.wait()

    @pl.loop(0, 2)
    def _(n):
        columns = pl.ds(pl.multiple_of(n * 256, 256), 256)
        out[:, columns] = project_tile(table, 64, held, columns, tokens)


def project_long_kv(table, long_rows, pieces):
    return pl.pallas_call(
        long_kv_kernel,
        in_specs=[SMEM_SPEC, VMEM_SPEC] + [HBM_SPEC] * 8,
        out_specs=VMEM_SPEC,
        out_shape=jax.ShapeDtypeStruct((384, 512), jnp.bfloat16),
        scratch_shapes=[VMEM((64, 64, 512), jnp.bfloat16), pltpu.SemaphoreType.DMA((8,))],
        compiler_params=pltpu.CompilerParams(vmem_limit_bytes=10 << 20),
        cost_estimate=pl.CostEstimate(
            flops=2 * 384 * 4096 * 512, bytes_accessed=8 << 20, transcendentals=0
        ),
    )(table, long_rows, *pieces)


def short_places():
    core = lax.axis_index("uly")
    return pl.multiple_of(core * 512, 512), pl.multiple_of(512 - core * 512, 512)


def short_kv_kernel(table, own, partner, *refs):
    pieces = refs[:8]
    out, held, sems = refs[8:]
    first, other = short_places()
    for copy in load(pieces, held, sems):
        copy.wait()

    @pl.loop(0, 2)
    def _(n):
        columns = pl.ds(pl.multiple_of(n * 256, 256), 256)
        out[pl.ds(first, 512), columns] = project_tile(table, 64, held, columns, own)
        out[pl.ds(other, 512), columns] = project_tile(table, 64, held, columns, partner)


def project_short_kv(table, own, partner, pieces):
    return pl.pallas_call(
        short_kv_kernel,
        in_specs=[SMEM_SPEC, VMEM_SPEC, VMEM_SPEC] + [HBM_SPEC] * 8,
        out_specs=VMEM_SPEC,
        out_shape=jax.ShapeDtypeStruct((1024, 512), jnp.bfloat16),
        scratch_shapes=[VMEM((64, 64, 512), jnp.bfloat16), pltpu.SemaphoreType.DMA((8,))],
        compiler_params=pltpu.CompilerParams(vmem_limit_bytes=10 << 20),
        cost_estimate=pl.CostEstimate(
            flops=2 * 1024 * 4096 * 512, bytes_accessed=14 << 20, transcendentals=0
        ),
    )(table, own, partner, *pieces)


def queries_kernel(table, own, partner, long, *refs):
    pieces = refs[:8]
    out, out_long, held, sems = refs[8:]
    first, other = short_places()
    for copy in load(pieces, held, sems):
        copy.wait()

    @pl.loop(0, 4)
    def _(n):
        columns = pl.ds(pl.multiple_of(n * 256, 256), 256)
        out[pl.ds(first, 512), columns] = project_tile(table, 0, held, columns, own)
        out[pl.ds(other, 512), columns] = project_tile(table, 0, held, columns, partner)
        out_long[:, columns] = project_tile(table, 0, held, columns, long)


def project_queries(table, own, partner, long_rows, pieces):
    return pl.pallas_call(
        queries_kernel,
        in_specs=[SMEM_SPEC] + [VMEM_SPEC] * 3 + [HBM_SPEC] * 8,
        out_specs=[VMEM_SPEC] * 2,
        out_shape=[
            jax.ShapeDtypeStruct((1024, 1024), jnp.bfloat16),
            jax.ShapeDtypeStruct((384, 1024), jnp.bfloat16),
        ],
        scratch_shapes=[VMEM((64, 64, 1024), jnp.bfloat16), pltpu.SemaphoreType.DMA((8,))],
        compiler_params=pltpu.CompilerParams(vmem_limit_bytes=16 << 20),
        cost_estimate=pl.CostEstimate(
            flops=2 * 1408 * 4096 * 1024, bytes_accessed=24 << 20, transcendentals=0
        ),
    )(table, own, partner, long_rows, *pieces)


QUERY_ROWS = 128
NT = (((1,), (1,)), ((), ()))


def short_kernel(seg_row, seg_col, queries, keys, values, out):
    for block in range(1024 // QUERY_ROWS):
        first = block * QUERY_ROWS
        start = max(0, first - 512)
        end = first + QUERY_ROWS
        width = end - start
        same = seg_col[first:end, 0:1] == seg_row[0:1, start:end]
        query_pos = first + lax.broadcasted_iota(jnp.int32, (QUERY_ROWS, width), 0)
        key_pos = start + lax.broadcasted_iota(jnp.int32, (QUERY_ROWS, width), 1)
        bias = jnp.where(same & (key_pos <= query_pos), 0.0, HIDDEN)
        heads = jnp.concatenate(
            [queries[first:end, h * HD : (h + 1) * HD] for h in range(4)], axis=0
        )
        scores = lax.dot_general(
            heads, keys[start:end, :], NT, preferred_element_type=jnp.float32
        )
        scores = scores.reshape(4, QUERY_ROWS, width) + bias[None]
        top = jnp.max(scores, axis=-1, keepdims=True)
        exponentials = jnp.exp2((scores - top) * EXP_SCALE)
        totals = jnp.sum(exponentials, axis=-1, keepdims=True)
        mixed = jnp.dot(
            exponentials.astype(jnp.bfloat16).reshape(4 * QUERY_ROWS, width),
            values[start:end, :],
            preferred_element_type=jnp.float32,
        ).reshape(4, QUERY_ROWS, HD)
        mixed = (mixed * (1.0 / totals)).astype(jnp.bfloat16)
        for h in range(4):
            out[first:end, h * HD : (h + 1) * HD] = mixed[h]


def short_attention(segments, queries, kv):
    seg_col = jnp.broadcast_to(segments.reshape(1024, 1), (1024, 128))
    return pl.pallas_call(
        short_kernel,
        grid=(2,),
        in_specs=[
            pl.BlockSpec((1, 1024), lambda g: (0, 0)),
            pl.BlockSpec((1024, 128), lambda g: (0, 0)),
            pl.BlockSpec((1024, 512), lambda g: (0, g)),
            pl.BlockSpec((1024, 128), lambda g: (0, g)),
            pl.BlockSpec((1024, 128), lambda g: (0, 2 + g)),
        ],
        out_specs=pl.BlockSpec((1024, 512), lambda g: (0, g)),
        out_shape=jax.ShapeDtypeStruct((1024, 1024), jnp.bfloat16),
        compiler_params=pltpu.CompilerParams(vmem_limit_bytes=24 << 20),
        cost_estimate=pl.CostEstimate(
            flops=8 * 1024 * 640 * 512, bytes_accessed=6 << 20, transcendentals=8 * 1024 * 640
        ),
    )(segments, seg_col, queries, kv, kv)


LONG_ROWS = 384


def long_kernel(place, queries, *refs):
    pieces = refs[:8]
    out, held, top, total, mixed, sems = refs[8:]
    copies = [
        pltpu.make_async_copy(piece, held.at[i], sems.at[i]) for i, piece in enumerate(pieces)
    ]
    for copy in copies:
        copy.start()
    for copy in copies:
        copy.wait()
    block = place[0]
    length = place[1]
    first = block * LONG_ROWS
    live = first < length

    def visit(slot, group, diagonal):
        heads = jnp.concatenate(
            [queries[:, (4 * group + h) * HD : (4 * group + h + 1) * HD] for h in range(4)],
            axis=0,
        )
        scores = lax.dot_general(
            heads,
            held[slot, :, group * HD : (group + 1) * HD],
            NT,
            preferred_element_type=jnp.float32,
        )
        if diagonal:
            square = (LONG_ROWS, LONG_ROWS)
            causal = lax.broadcasted_iota(jnp.int32, square, 1) <= lax.broadcasted_iota(
                jnp.int32, square, 0
            )
            bias = jnp.where(causal, 0.0, HIDDEN)
            scores = (scores.reshape(4, *square) + bias[None]).reshape(4 * LONG_ROWS, LONG_ROWS)
        largest = jnp.max(scores, axis=-1, keepdims=True)
        if diagonal:
            new = jnp.broadcast_to(largest, (4 * LONG_ROWS, HD))
        else:
            old = top[group]
            new = jnp.maximum(old, largest)
            rescale = jnp.exp2((old - new) * EXP_SCALE)
        parts = [jnp.exp2((scores[:, k : k + HD] - new) * EXP_SCALE) for k in range(0, 384, HD)]
        summed = parts[0] + parts[1] + parts[2]
        weighted = jnp.dot(
            jnp.concatenate([part.astype(jnp.bfloat16) for part in parts], axis=1),
            held[slot, :, 256 + group * HD : 256 + (group + 1) * HD],
            preferred_element_type=jnp.float32,
        )
        top[group] = new
        if diagonal:
            total[group] = summed
            mixed[group] = weighted
        else:
            total[group] = total[group] * rescale + summed
            mixed[group] = mixed[group] * rescale + weighted

    @pl.when(live)
    def _():
        for group in range(2):
            visit(0, group, True)

        @pl.loop(0, block)
        def _(index):
            for group in range(2):
                visit(place[2 + index], group, False)

        position = first + lax.broadcasted_iota(jnp.int32, (LONG_ROWS, HD), 0)
        for group in range(2):
            done = mixed[group] * (1.0 / jnp.sum(total[group], axis=-1, keepdims=True))
            for h in range(4):
                head = 4 * group + h
                out[:, head * HD : (head + 1) * HD] = jnp.where(
                    position < length, done[h * LONG_ROWS : (h + 1) * LONG_ROWS], 0.0
                ).astype(jnp.bfloat16)

    @pl.when(jnp.logical_not(live))
    def _():
        out[...] = jnp.zeros_like(out)


def long_attention(place, queries, kv_pieces):
    return pl.pallas_call(
        long_kernel,
        in_specs=[SMEM_SPEC, VMEM_SPEC] + [HBM_SPEC] * 8,
        out_specs=VMEM_SPEC,
        out_shape=jax.ShapeDtypeStruct((LONG_ROWS, 1024), jnp.bfloat16),
        scratch_shapes=[VMEM((8, LONG_ROWS, 512), jnp.bfloat16)]
        + [VMEM((2, 4 * LONG_ROWS, HD), jnp.float32)] * 3
        + [pltpu.SemaphoreType.DMA((8,))],
        compiler_params=pltpu.CompilerParams(vmem_limit_bytes=28 << 20),
        cost_estimate=pl.CostEstimate(
            flops=8 * 384 * 3072 * 512, bytes_accessed=6 << 20, transcendentals=8 * 384 * 3072
        ),
    )(place, queries, *kv_pieces)


X_DIMS = (0, 0)


def exchange_kv(kv):
    other = swap_y_lo(kv)
    kv_after = shift(kv, X_DIMS, -1)
    kv_before = shift(kv, X_DIMS, 1)
    other_after = shift(other, X_DIMS, -1)
    other_before = shift(other, X_DIMS, 1)
    kv_far = shift(kv_before, X_DIMS, 1)
    other_far = shift(other_after, X_DIMS, -1)
    return kv, other, kv_after, other_after, kv_far, other_far, kv_before, other_before


def body(short_tokens, short_segments, long_tokens, long_lengths, w_query, w_key, w_value):
    short_rows = short_tokens[0]
    long_rows = long_tokens[0]
    core = lax.axis_index("uly")
    blk = lax.axis_index("blk").astype(jnp.int32)
    dp = lax.axis_index("dp").astype(jnp.int32)
    coords = (blk // 2, (dp % 2) * 2 + blk % 2, dp // 2)
    table = block_table(coords, core)
    index = jnp.arange(8, dtype=jnp.int32)
    slots = ((index // 2 - blk // 2) & 3) * 2 + ((index ^ blk) & 1)
    place = jnp.concatenate([blk[None], long_lengths, slots])
    kv_weights = jnp.concatenate((w_key, w_value), axis=1)
    partner_rows = lax.ppermute(short_rows, "uly", [(0, 1), (1, 0)])
    query_pieces, kv_pieces = gather_weights(w_query, kv_weights)
    long_kv = project_long_kv(table, long_rows, kv_pieces)
    long_pieces = exchange_kv(long_kv)
    kv = project_short_kv(table, short_rows, partner_rows, kv_pieces)
    queries, long_queries = project_queries(
        table, short_rows, partner_rows, long_rows, query_pieces
    )
    attended = short_attention(short_segments, queries, kv)
    mine = lax.dynamic_slice_in_dim(attended, core * 512, 512, axis=0)
    theirs = lax.dynamic_slice_in_dim(attended, 512 - core * 512, 512, axis=0)
    other = lax.ppermute(theirs, "uly", [(0, 1), (1, 0)])
    long_out = long_attention(place, long_queries, long_pieces)
    short_out = jnp.concatenate(
        [jnp.where(core == 0, mine, other), jnp.where(core == 0, other, mine)], axis=1
    )
    return short_out[None], long_out[None]


def solution(mesh):
    return jax.shard_map(
        body,
        mesh=mesh,
        in_specs=(
            P(("blk", "dp"), "uly", None),
            P(("blk", "dp"), None),
            P("dp", "blk", None),
            P("dp"),
            P(("blk", "dp"), "uly"),
            P(("blk", "dp"), "uly"),
            P(("blk", "dp"), "uly"),
        ),
        out_specs=(P(("blk", "dp"), "uly", None), P("dp", "blk", "uly")),
        check_vma=False,
    )
```

```python
import functools
import itertools
import math

import jax
import jax.numpy as jnp
from jax import lax
from jax.experimental import pallas as pl
from jax.experimental.pallas import tpu as pltpu
from jax.sharding import PartitionSpec as P


HD = 128
HIDDEN = -1e30
EXP_SCALE = math.log2(math.e) / math.sqrt(HD)
VMEM = pltpu.VMEM


ALL_AXES = ("blk", "uly", "dp")
QUERY_DIMS = ((2, 1, 0), (0, 2, 1))
KV_DIMS = ((1, 0, 2), (1, 0, 2))


def device_index(x, y, z, core):
    return ((x * 2 + y % 2) * 2 + core) * 8 + z * 2 + y // 2


def shift(rows, dims, hops):
    pairs = []
    for core in range(2):
        for at in itertools.product(range(4), repeat=3):
            to = list(at)
            to[dims[core]] = (to[dims[core]] + hops) % 4
            pairs.append((device_index(*at, core), device_index(*to, core)))
    return lax.ppermute(rows, ALL_AXES, pairs)


def swap_y_lo(rows):
    pairs = []
    for core in range(2):
        for x, y, z in itertools.product(range(4), repeat=3):
            pairs.append((device_index(x, y, z, core), device_index(x, y ^ 1, z, core)))
    return lax.ppermute(rows, ALL_AXES, pairs)


SMEM_SPEC = pl.BlockSpec(memory_space=pltpu.SMEM)
VMEM_SPEC = pl.BlockSpec(memory_space=VMEM)
HBM_SPEC = pl.BlockSpec(memory_space=pltpu.HBM)


def pack_kernel(parts, *refs):
    outs = refs[-len(parts) :]
    at = 0
    for out, count in zip(outs, parts):
        row = 0
        for ref in refs[at : at + count]:
            out[row : row + ref.shape[0], :] = ref[...]
            row += ref.shape[0]
        at += count


def pack(*groups):
    parts = tuple(len(group) for group in groups)
    flat = [piece for group in groups for piece in group]
    shapes = [
        jax.ShapeDtypeStruct((sum(p.shape[0] for p in group), group[0].shape[1]), jnp.bfloat16)
        for group in groups
    ]
    size = sum(piece.size for piece in flat) * 4
    return pl.pallas_call(
        functools.partial(pack_kernel, parts),
        in_specs=[VMEM_SPEC] * len(flat),
        out_specs=[VMEM_SPEC] * len(parts),
        out_shape=shapes,
        compiler_params=pltpu.CompilerParams(vmem_limit_bytes=8 << 20),
        cost_estimate=pl.CostEstimate(flops=size, bytes_accessed=size, transcendentals=0),
    )(*flat)


def direct_ring(rows, dims):
    return rows, shift(rows, dims, -1), shift(rows, dims, 2), shift(rows, dims, 1)


def passed_ring(rows, dims):
    after = shift(rows, dims, -1)
    before = shift(rows, dims, 1)
    far = shift(after, dims, -1)
    return (rows, after), (far, before)


def halved_ring(low, high, dims):
    before_low = shift(low, dims, 1)
    after_low = shift(low, dims, -1)
    before_high = shift(high, dims, 1)
    after_high = shift(high, dims, -1)
    far_low = shift(before_low, dims, 1)
    far_high = shift(after_high, dims, -1)
    near = (after_low, after_high, before_low, before_high)
    rest = (low, high, far_low, far_high)
    return [
        tuple(piece.reshape(8, 64, piece.shape[1]) for piece in pieces) for pieces in (near, rest)
    ]


def gather_weights(w_query, kv_weights):
    query_dims, kv_dims = tuple(zip(*QUERY_DIMS)), tuple(zip(*KV_DIMS))
    queries, kv = pack(direct_ring(w_query, query_dims[0]), direct_ring(kv_weights, kv_dims[0]))
    query_two = passed_ring(queries, query_dims[1])
    kv_two = passed_ring(kv, kv_dims[1])
    query_low, kv_low = pack(query_two[0], kv_two[0])
    query_high, kv_high = pack(query_two[1], kv_two[1])
    query_pieces = halved_ring(query_low, query_high, query_dims[2])
    kv_pieces = halved_ring(kv_low, kv_high, kv_dims[2])
    return query_pieces, kv_pieces


def unit_table(coords, core):
    x, y, z = coords
    t = jnp.arange(32, dtype=jnp.int32)
    away, r = 1 - t // 16, t % 16
    first = core == 0
    query_x = jnp.where(first, (x + away + 2 * (r // 8)) & 3, r // 4)
    query_y_lo = jnp.where(first, (r // 4) & 1, (y ^ away) & 1)
    kv_z = (z + away + 2 * (r & 1)) & 3

    def blocks(at_x, at_y_lo, at_z, dims):
        rows = []
        for y_hi in range(2):
            at = (at_x, y_hi * 2 + at_y_lo, at_z)
            steps = [(at[d] - coords[d]) & 3 for d in dims]
            rows.append((steps[2] // 2) * 16 + steps[1] * 4 + steps[0])
        return jnp.stack(rows, axis=1).reshape(64)

    query_at = (query_x, query_y_lo, r & 3)
    kv_at = (r // 4, (r // 2) & 1, kv_z)
    query_blocks = jnp.where(
        first, blocks(*query_at, QUERY_DIMS[0]), blocks(*query_at, QUERY_DIMS[1])
    )
    columns = [at_x * 8 + at_y_lo * 4 + at_z for at_x, at_y_lo, at_z in (query_at, kv_at)]
    return jnp.concatenate(columns + [query_blocks, blocks(*kv_at, KV_DIMS[0])])


QUERY, KV = 0, 1
NEAR, REST = 0, 1


def piece_copies(pieces, held, sems):
    copies, at = [], 0
    for i, piece in enumerate(pieces):
        count = piece.shape[0]
        copies.append(pltpu.make_async_copy(piece, held.at[at : at + count], sems.at[i]))
        at += count
    return copies


def load(pieces, held, sems):
    copies = piece_copies(pieces, held, sems)
    for copy in copies:
        copy.start()
    return copies


def wait_all(copies):
    for copy in copies:
        copy.wait()


def place_rows(table, kind, half, held, columns, ordered):
    for r in range(32):
        block = table[64 + 64 * kind + 32 * half + r]
        ordered[64 * r : 64 * (r + 1), :] = held[block, :, columns]


def half_depth(table, kind, half, tokens, ordered):
    units = []
    for u in range(16):
        at = pl.multiple_of(table[32 * kind + 16 * half + u] * 128, 128)
        units.append(tokens[:, pl.ds(at, 128)])
    return jnp.dot(
        jnp.concatenate(units, axis=1), ordered[...], preferred_element_type=jnp.float32
    )


WIDE = 512


def wide_columns(n):
    return pl.ds(pl.multiple_of(n * WIDE, WIDE), WIDE)


def near_kernel(table, own, partner, long, *refs):
    kv_pieces, query_pieces = refs[:4], refs[4:8]
    kv_short, kv_long, q_short, q_long, held_kv, held_q, ordered, sems = refs[8:15] + refs[-1:]
    first, second = refs[15:17]
    kv_copies = load(kv_pieces, held_kv, sems.at[0])
    tokens = [
        pltpu.make_async_copy(own, first, sems.at[2, 0]),
        pltpu.make_async_copy(partner, second, sems.at[2, 1]),
    ]
    tokens[0].start()
    tokens[1].start()
    query_copies = load(query_pieces, held_q, sems.at[1])
    wait_all(kv_copies)
    place_rows(table, KV, NEAR, held_kv, slice(None), ordered)
    kv_long[...] = half_depth(table, KV, NEAR, long, ordered)
    tokens[0].wait()
    kv_short[0:512, :] = half_depth(table, KV, NEAR, first, ordered)
    tokens[1].wait()
    kv_short[512:1024, :] = half_depth(table, KV, NEAR, second, ordered)
    wait_all(query_copies)

    @pl.loop(0, 2)
    def _(n):
        columns = wide_columns(n)
        place_rows(table, QUERY, NEAR, held_q, columns, ordered)
        q_long[:, columns] = half_depth(table, QUERY, NEAR, long, ordered)
        q_short[0:512, columns] = half_depth(table, QUERY, NEAR, first, ordered)
        q_short[512:1024, columns] = half_depth(table, QUERY, NEAR, second, ordered)


def project_near(table, own, partner, long_rows, kv_near, query_near):
    return pl.pallas_call(
        near_kernel,
        in_specs=[SMEM_SPEC] + [HBM_SPEC] * 2 + [VMEM_SPEC] + [HBM_SPEC] * 8,
        out_specs=[VMEM_SPEC] * 4,
        out_shape=[
            jax.ShapeDtypeStruct((1024, 512), jnp.float32),
            jax.ShapeDtypeStruct((384, 512), jnp.float32),
            jax.ShapeDtypeStruct((1024, 1024), jnp.float32),
            jax.ShapeDtypeStruct((384, 1024), jnp.float32),
        ],
        scratch_shapes=[
            VMEM((32, 64, 512), jnp.bfloat16),
            VMEM((32, 64, 1024), jnp.bfloat16),
            VMEM((2048, WIDE), jnp.bfloat16),
            VMEM((512, 4096), jnp.bfloat16),
            VMEM((512, 4096), jnp.bfloat16),
            pltpu.SemaphoreType.DMA((3, 4)),
        ],
        compiler_params=pltpu.CompilerParams(vmem_limit_bytes=24 << 20),
        cost_estimate=pl.CostEstimate(
            flops=1408 * 4096 * 1536, bytes_accessed=24 << 20, transcendentals=0
        ),
    )(table, own, partner, long_rows, *kv_near, *query_near)


def long_kv_kernel(table, tokens, near, *refs):
    out, held, ordered, sems = refs[4:]
    wait_all(load(refs[:4], held, sems))
    place_rows(table, KV, REST, held, slice(None), ordered)
    out[...] = (near[...] + half_depth(table, KV, REST, tokens, ordered)).astype(jnp.bfloat16)


REST_KV_SCRATCH = (
    VMEM((32, 64, 512), jnp.bfloat16),
    VMEM((2048, WIDE), jnp.bfloat16),
    pltpu.SemaphoreType.DMA((4,)),
)


def project_long_kv(table, long_rows, near, pieces):
    return pl.pallas_call(
        long_kv_kernel,
        in_specs=[SMEM_SPEC, VMEM_SPEC, VMEM_SPEC] + [HBM_SPEC] * 4,
        out_specs=VMEM_SPEC,
        out_shape=jax.ShapeDtypeStruct((384, 512), jnp.bfloat16),
        scratch_shapes=REST_KV_SCRATCH,
        compiler_params=pltpu.CompilerParams(vmem_limit_bytes=9 << 20),
        cost_estimate=pl.CostEstimate(
            flops=384 * 4096 * 512, bytes_accessed=6 << 20, transcendentals=0
        ),
    )(table, long_rows, near, *pieces)


def short_places():
    core = lax.axis_index("uly")
    return pl.multiple_of(core * 512, 512), pl.multiple_of(512 - core * 512, 512)


def short_kv_kernel(table, own, partner, near, *refs):
    out, held, ordered, sems, second, second_sem = refs[4:]
    first, other = short_places()
    copies = load(refs[:4], held, sems)
    copy = pltpu.make_async_copy(partner, second, second_sem)
    copy.start()
    wait_all(copies)
    place_rows(table, KV, REST, held, slice(None), ordered)
    out[pl.ds(first, 512), :] = (
        near[0:512, :] + half_depth(table, KV, REST, own, ordered)
    ).astype(jnp.bfloat16)
    copy.wait()
    out[pl.ds(other, 512), :] = (
        near[512:1024, :] + half_depth(table, KV, REST, second, ordered)
    ).astype(jnp.bfloat16)


def project_short_kv(table, own, partner, near, pieces):
    return pl.pallas_call(
        short_kv_kernel,
        in_specs=[SMEM_SPEC, VMEM_SPEC, HBM_SPEC, VMEM_SPEC] + [HBM_SPEC] * 4,
        out_specs=VMEM_SPEC,
        out_shape=jax.ShapeDtypeStruct((1024, 512), jnp.bfloat16),
        scratch_shapes=REST_KV_SCRATCH
        + (VMEM((512, 4096), jnp.bfloat16), pltpu.SemaphoreType.DMA),
        compiler_params=pltpu.CompilerParams(vmem_limit_bytes=16 << 20),
        cost_estimate=pl.CostEstimate(
            flops=1024 * 4096 * 512, bytes_accessed=12 << 20, transcendentals=0
        ),
    )(table, own, partner, near, *pieces)


def queries_kernel(table, own, partner, long, near, near_long, *refs):
    pieces = refs[:4]
    out, out_long, held, ordered, second, sems, second_sem = refs[4:]
    first, other = short_places()

    def piece_loads(n):
        columns = slice(n * WIDE, (n + 1) * WIDE)
        return [
            pltpu.make_async_copy(
                piece.at[:, :, columns], held.at[n, 8 * i : 8 * (i + 1)], sems.at[n, i]
            )
            for i, piece in enumerate(pieces)
        ]

    copy = pltpu.make_async_copy(partner, second, second_sem)
    for load in piece_loads(0) + [copy] + piece_loads(1):
        load.start()
    for n in range(2):
        columns = slice(n * WIDE, (n + 1) * WIDE)
        wait_all(piece_loads(n))
        place_rows(table, QUERY, REST, held.at[n], slice(None), ordered)
        out_long[:, columns] = (
            near_long[:, columns] + half_depth(table, QUERY, REST, long, ordered)
        ).astype(jnp.bfloat16)
        out[pl.ds(first, 512), columns] = (
            near[0:512, columns] + half_depth(table, QUERY, REST, own, ordered)
        ).astype(jnp.bfloat16)
        if n == 0:
            copy.wait()
        out[pl.ds(other, 512), columns] = (
            near[512:1024, columns] + half_depth(table, QUERY, REST, second, ordered)
        ).astype(jnp.bfloat16)


def project_queries(table, own, partner, long_rows, near, near_long, pieces):
    return pl.pallas_call(
        queries_kernel,
        in_specs=[SMEM_SPEC, VMEM_SPEC, HBM_SPEC] + [VMEM_SPEC] * 3 + [HBM_SPEC] * 4,
        out_specs=[VMEM_SPEC] * 2,
        out_shape=[
            jax.ShapeDtypeStruct((1024, 1024), jnp.bfloat16),
            jax.ShapeDtypeStruct((384, 1024), jnp.bfloat16),
        ],
        scratch_shapes=[
            VMEM((2, 32, 64, WIDE), jnp.bfloat16),
            VMEM((2048, WIDE), jnp.bfloat16),
            VMEM((512, 4096), jnp.bfloat16),
            pltpu.SemaphoreType.DMA((2, 4)),
            pltpu.SemaphoreType.DMA,
        ],
        compiler_params=pltpu.CompilerParams(vmem_limit_bytes=20 << 20),
        cost_estimate=pl.CostEstimate(
            flops=1408 * 4096 * 1024, bytes_accessed=24 << 20, transcendentals=0
        ),
    )(table, own, partner, long_rows, near, near_long, *pieces)


QUERY_ROWS = 128
NT = (((1,), (1,)), ((), ()))


def lanes(start, size):
    return pl.ds(pl.multiple_of(start, HD), size)


def short_kernel(seg_row, seg_col, queries, kv, mine, theirs, held, sems):
    first_row, other_row = short_places()

    def copies(group):
        columns = lanes(group * 512, 512)
        return [
            pltpu.make_async_copy(
                held.at[pl.ds(rows, 512), columns], out.at[:, columns], sems.at[group, i]
            )
            for i, (rows, out) in enumerate(((first_row, mine), (other_row, theirs)))
        ]

    @pl.loop(0, 2)
    def _(group):
        for block in range(1024 // QUERY_ROWS):
            short_block(seg_row, seg_col, queries, kv, held, group, block)
        for copy in copies(group):
            copy.start()

    wait_all(copies(0) + copies(1))


def short_block(seg_row, seg_col, queries, kv, out, group, block):
    first = block * QUERY_ROWS
    start = max(0, first - 512)
    end = first + QUERY_ROWS
    width = end - start
    same = seg_col[first:end, 0:1] == seg_row[0:1, start:end]
    query_pos = first + lax.broadcasted_iota(jnp.int32, (QUERY_ROWS, width), 0)
    key_pos = start + lax.broadcasted_iota(jnp.int32, (QUERY_ROWS, width), 1)
    bias = jnp.where(same & (key_pos <= query_pos), 0.0, HIDDEN)
    columns = [lanes(group * 512 + h * HD, HD) for h in range(4)]
    heads = jnp.concatenate([queries[first:end, c] for c in columns], axis=0)
    keys = kv[start:end, lanes(group * HD, HD)]
    values = kv[start:end, lanes(256 + group * HD, HD)]
    scores = lax.dot_general(heads, keys, NT, preferred_element_type=jnp.float32)
    scores = scores.reshape(4, QUERY_ROWS, width) + bias[None]
    top = jnp.max(scores, axis=-1, keepdims=True)
    exponentials = jnp.exp2((scores - top) * EXP_SCALE)
    totals = jnp.sum(exponentials, axis=-1, keepdims=True)
    mixed = jnp.dot(
        exponentials.astype(jnp.bfloat16).reshape(4 * QUERY_ROWS, width),
        values,
        preferred_element_type=jnp.float32,
    ).reshape(4, QUERY_ROWS, HD)
    mixed = (mixed * (1.0 / totals)).astype(jnp.bfloat16)
    for h, c in enumerate(columns):
        out[first:end, c] = mixed[h]


def short_attention(segments, seg_col, queries, kv):
    return pl.pallas_call(
        short_kernel,
        in_specs=[VMEM_SPEC] * 4,
        out_specs=[HBM_SPEC] * 2,
        out_shape=[jax.ShapeDtypeStruct((512, 1024), jnp.bfloat16)] * 2,
        scratch_shapes=[VMEM((1024, 1024), jnp.bfloat16), pltpu.SemaphoreType.DMA((2, 2))],
        compiler_params=pltpu.CompilerParams(vmem_limit_bytes=24 << 20),
        cost_estimate=pl.CostEstimate(
            flops=8 * 1024 * 640 * 512, bytes_accessed=6 << 20, transcendentals=8 * 1024 * 640
        ),
    )(segments, seg_col, queries, kv)


LONG_ROWS = 384
VISIT = 512


def long_kernel(place, queries, mine, *refs):
    pieces = refs[:8]
    out, short_out, held, heads, top, total, mixed, half, sems, half_sem = refs[8:]
    block, length = place[0], place[1]
    copies = []
    for i, piece in enumerate(pieces):
        at = ((block // 2 + i // 2) & 3) * 2 + ((block & 1) ^ (i % 2))
        rows = pl.ds(pl.multiple_of(at * LONG_ROWS, LONG_ROWS), LONG_ROWS)
        copies.append(pltpu.make_async_copy(piece, held.at[rows], sems.at[i]))
    half_in = pltpu.make_async_copy(mine, half, half_sem.at[0])
    for copy in copies + [half_in]:
        copy.start()
    core = lax.axis_index("uly")
    half_out = pltpu.make_async_copy(half, short_out.at[:, lanes(core * 1024, 1024)], half_sem.at[1])
    first = block * LONG_ROWS
    live = first < length
    for head in range(8):
        rows = slice((head % 4) * LONG_ROWS, (head % 4 + 1) * LONG_ROWS)
        heads[head // 4, rows, :] = queries[:, head * HD : (head + 1) * HD]
    top[...] = jnp.full_like(top, HIDDEN)
    total[...] = jnp.zeros_like(total)
    mixed[...] = jnp.zeros_like(mixed)
    half_in.wait()
    half_out.start()
    wait_all(copies)

    def score(rows, group, bias):
        scores = lax.dot_general(
            heads[group],
            held[rows, group * HD : (group + 1) * HD],
            NT,
            preferred_element_type=jnp.float32,
        )
        if bias is not None:
            scores = scores.reshape(4, LONG_ROWS, VISIT) + bias[None]
            scores = scores.reshape(4 * LONG_ROWS, VISIT)
        return scores

    def add(rows, group, scores):
        old = top[group]
        new = jnp.maximum(old, jnp.max(scores, axis=-1, keepdims=True))
        rescale = jnp.exp2((old - new) * EXP_SCALE)
        parts = [jnp.exp2((scores[:, k : k + HD] - new) * EXP_SCALE) for k in range(0, VISIT, HD)]
        top[group] = new
        total[group] = total[group] * rescale + ((parts[0] + parts[1]) + (parts[2] + parts[3]))
        weighted = jnp.dot(
            jnp.concatenate([part.astype(jnp.bfloat16) for part in parts], axis=1),
            held[rows, 256 + group * HD : 256 + (group + 1) * HD],
            preferred_element_type=jnp.float32,
        )
        mixed[group] = mixed[group] * rescale + weighted

    def visit(index, bias):
        rows = pl.ds(pl.multiple_of(index * VISIT, VISIT), VISIT)
        scores = score(rows, 0, bias)
        later = score(rows, 1, bias)
        add(rows, 0, scores)
        add(rows, 1, later)

    @pl.when(live)
    def _():
        @pl.loop(0, first // VISIT)
        def _(index):
            visit(index, None)

        @pl.loop(first // VISIT, (first + LONG_ROWS - 1) // VISIT + 1)
        def _(index):
            square = (LONG_ROWS, VISIT)
            key_pos = index * VISIT + lax.broadcasted_iota(jnp.int32, square, 1)
            query_pos = first + lax.broadcasted_iota(jnp.int32, square, 0)
            visit(index, jnp.where(key_pos <= query_pos, 0.0, HIDDEN))

        position = first + lax.broadcasted_iota(jnp.int32, (LONG_ROWS, HD), 0)
        for group in range(2):
            done = mixed[group] * (1.0 / jnp.sum(total[group], axis=-1, keepdims=True))
            for h in range(4):
                head = 4 * group + h
                out[:, head * HD : (head + 1) * HD] = jnp.where(
                    position < length, done[h * LONG_ROWS : (h + 1) * LONG_ROWS], 0.0
                ).astype(jnp.bfloat16)

    @pl.when(jnp.logical_not(live))
    def _():
        out[...] = jnp.zeros_like(out)

    half_out.wait()


def long_attention(place, queries, mine, pieces):
    state = VMEM((2, 4 * LONG_ROWS, HD), jnp.float32)
    return pl.pallas_call(
        long_kernel,
        in_specs=[SMEM_SPEC, VMEM_SPEC] + [HBM_SPEC] * 9,
        out_specs=[VMEM_SPEC, HBM_SPEC],
        out_shape=[
            jax.ShapeDtypeStruct((LONG_ROWS, 1024), jnp.bfloat16),
            jax.ShapeDtypeStruct((512, 2048), jnp.bfloat16),
        ],
        scratch_shapes=[
            VMEM((8 * LONG_ROWS, 512), jnp.bfloat16),
            VMEM((2, 4 * LONG_ROWS, HD), jnp.bfloat16),
            state,
            state,
            state,
            VMEM((512, 1024), jnp.bfloat16),
            pltpu.SemaphoreType.DMA((8,)),
            pltpu.SemaphoreType.DMA((2,)),
        ],
        compiler_params=pltpu.CompilerParams(vmem_limit_bytes=36 << 20),
        cost_estimate=pl.CostEstimate(
            flops=8 * 384 * 3072 * 512, bytes_accessed=6 << 20, transcendentals=8 * 384 * 3072
        ),
    )(place, queries, mine, *pieces)


def other_half_kernel(other, unused, short_out, half, sems):
    core = lax.axis_index("uly")
    inward = pltpu.make_async_copy(other, half, sems.at[0])
    inward.start()
    inward.wait()
    columns = lanes((1 - core) * 1024, 1024)
    outward = pltpu.make_async_copy(half, short_out.at[:, columns], sems.at[1])
    outward.start()
    outward.wait()


def add_other_half(other, short_out):
    return pl.pallas_call(
        other_half_kernel,
        in_specs=[HBM_SPEC] * 2,
        out_specs=HBM_SPEC,
        out_shape=jax.ShapeDtypeStruct((512, 2048), jnp.bfloat16),
        scratch_shapes=[VMEM((512, 1024), jnp.bfloat16), pltpu.SemaphoreType.DMA((2,))],
        input_output_aliases={1: 0},
        compiler_params=pltpu.CompilerParams(vmem_limit_bytes=4 << 20),
        cost_estimate=pl.CostEstimate(flops=1 << 20, bytes_accessed=4 << 20, transcendentals=0),
    )(other, short_out)


X_DIMS = (0, 0)


def exchange_kv(kv):
    other = swap_y_lo(kv)
    kv_after = shift(kv, X_DIMS, -1)
    kv_before = shift(kv, X_DIMS, 1)
    other_after = shift(other, X_DIMS, -1)
    other_before = shift(other, X_DIMS, 1)
    kv_far = shift(kv_before, X_DIMS, 1)
    other_far = shift(other_after, X_DIMS, -1)
    return kv, other, kv_after, other_after, kv_far, other_far, kv_before, other_before


def body(short_tokens, short_segments, long_tokens, long_lengths, w_query, w_key, w_value):
    short_rows = short_tokens[0]
    long_rows = long_tokens[0]
    core = lax.axis_index("uly")
    blk = lax.axis_index("blk").astype(jnp.int32)
    dp = lax.axis_index("dp").astype(jnp.int32)
    coords = (blk // 2, (dp % 2) * 2 + blk % 2, dp // 2)
    table = unit_table(coords, core)
    place = jnp.concatenate([blk[None], long_lengths])
    seg_col = jnp.broadcast_to(short_segments.reshape(1024, 1), (1024, 128))
    kv_weights = jnp.concatenate((w_key, w_value), axis=1)
    partner_rows = lax.ppermute(short_rows, "uly", [(0, 1), (1, 0)])
    (query_near, query_rest), (kv_near, kv_rest) = gather_weights(w_query, kv_weights)
    kv_short, kv_long, q_short, q_long = project_near(
        table, short_rows, partner_rows, long_rows, kv_near, query_near
    )
    long_kv = project_long_kv(table, long_rows, kv_long, kv_rest)
    long_pieces = exchange_kv(long_kv)
    kv = project_short_kv(table, short_rows, partner_rows, kv_short, kv_rest)
    queries, long_queries = project_queries(
        table, short_rows, partner_rows, long_rows, q_short, q_long, query_rest
    )
    mine, theirs = short_attention(short_segments, seg_col, queries, kv)
    other = lax.ppermute(theirs, "uly", [(0, 1), (1, 0)])
    long_out, short_out = long_attention(place, long_queries, mine, long_pieces)
    short_out = add_other_half(other, short_out)
    return short_out[None], long_out[None]


def solution(mesh):
    return jax.shard_map(
        body,
        mesh=mesh,
        in_specs=(
            P(("blk", "dp"), "uly", None),
            P(("blk", "dp"), None),
            P("dp", "blk", None),
            P("dp"),
            P(("blk", "dp"), "uly"),
            P(("blk", "dp"), "uly"),
            P(("blk", "dp"), "uly"),
        ),
        out_specs=(P(("blk", "dp"), "uly", None), P("dp", "blk", "uly")),
        check_vma=False,
    )
```
